32 devices in a mesh: io: 4 (over y, core), comp: 8 (over z, x).
Axes of the slice: x: 2, y: 2, z: 4, core: 2. Of those that a mesh axis runs over, the one named last changes fastest.
Arguments:
- fields: float32 [98304, 256], P(('io', 'comp')), may hold values from -6 to 6
- file_offset: int32 [768, 128], P(('io', 'comp')), may hold values from 0 to 98303, as said below
- level_remap: float32 [4, 64, 64], replicated, may hold values from -0.75 to 0.75
Outputs:
- history: float32 [98304, 256], P(('io', 'comp'))
The draws below stay inside these ranges and needn't reach their ends.
Inputs may be any that keep to these rules, and one draw needn't show every extreme that they name: file_offset is a permutation of the 98304 file positions. The owner of a position p is the device of flat index p // 3072 (io index times the comp size plus comp index). A device's columns have as owners only itself, devices of its io index and devices of its comp index. To each other device of its io index it sends exactly 8 columns, except the two of comp index one above and one below (cyclically), which get 8 plus between 96 and 192; likewise along io with the devices of its comp index. Two neighbours exchange equally many columns each way, and the count 8 + 192 is reached in every draw. Which columns and positions is drawn.
All inputs are finite; a program needn't handle non-finite values.
Results may differ from the reference program's by a relative error of at most 0.00005.
Values sent between devices are 32-bit elements; how exact they have to be, the bound alone decides.
A program may use at most 64 MiB of HBM per device.

```python
import jax
import jax.numpy as jnp
from jax import lax

FIELDS = 4
LEV = 64
COLS_DEV = 3072
SPREAD = 8
MOST = 192
COLS = 98304
N_IO = 4
N_COMP = 8


def draw_file_offset(key, part):
    group_count = N_IO
    task_count = N_COMP
    device_count = group_count * task_count
    keys = jax.random.split(jax.random.fold_in(key, 11), 7)
    lowest = MOST // 2
    comp_pairs = jax.random.randint(keys[0], (group_count, task_count), lowest, MOST + 1)
    comp_pairs = comp_pairs.at[jnp.arange(group_count), jax.random.randint(keys[1], (group_count,), 0, task_count)].set(MOST)
    io_pairs = jax.random.randint(keys[2], (group_count, task_count), lowest, MOST + 1)
    io_pairs = io_pairs.at[jax.random.randint(keys[3], (task_count,), 0, group_count), jnp.arange(task_count)].set(MOST)
    device = jnp.arange(device_count, dtype=jnp.int32)
    group = device // task_count
    task = device % task_count
    comp_targets = group[:, None] * task_count + jnp.arange(task_count, dtype=jnp.int32)[None, :]
    io_targets = jnp.arange(group_count, dtype=jnp.int32)[None, :] * task_count + task[:, None]
    near_targets = jnp.stack([group * task_count + (task + 1) % task_count, group * task_count + (task - 1) % task_count, (group + 1) % group_count * task_count + task, (group - 1) % group_count * task_count + task, device], axis=1)
    targets = jnp.concatenate([comp_targets, io_targets, near_targets], axis=1).astype(jnp.int32)
    spread_counts = jnp.full((device_count, task_count + group_count), SPREAD, jnp.int32)
    near_counts = jnp.stack([comp_pairs[group, task], comp_pairs[group, (task - 1) % task_count], io_pairs[group, task], io_pairs[(group - 1) % group_count, task]], axis=1).astype(jnp.int32)
    used = jnp.sum(spread_counts, axis=1) + jnp.sum(near_counts, axis=1)
    counts = jnp.concatenate([spread_counts, near_counts, (COLS_DEV - used)[:, None]], axis=1)
    ends = jnp.cumsum(counts, axis=1)
    position = jnp.arange(COLS_DEV, dtype=jnp.int32)
    segment = jax.vmap(lambda edge: jnp.searchsorted(edge, position, side='right'))(ends).astype(jnp.int32)
    owner = jnp.take_along_axis(targets, segment, axis=1)
    shuffles = jax.vmap(lambda k: jax.random.permutation(k, COLS_DEV))(jax.random.split(keys[4], device_count)).astype(jnp.int32)
    owner = jnp.take_along_axis(owner, shuffles, axis=1)
    flat_owner = owner.reshape(device_count * COLS_DEV)
    mixing = jax.random.permutation(keys[5], device_count * COLS_DEV).astype(jnp.int32)
    order = jnp.argsort(flat_owner[mixing], stable=True).astype(jnp.int32)
    offsets = jnp.zeros((device_count * COLS_DEV,), jnp.int32).at[mixing[order]].set(jnp.arange(device_count * COLS_DEV, dtype=jnp.int32))
    return offsets.reshape(device_count * COLS_DEV // 128, 128).astype(jnp.int32)


def shard_levels(rng, dims, cuts, low, largest):
    def one(axis_at, shards_of):
        steps = jax.random.uniform(jax.random.fold_in(jax.random.fold_in(rng, 6), axis_at), (shards_of,), jnp.float32, low / len(cuts), largest / len(cuts))
        return jnp.repeat(jnp.exp(steps), dims[axis_at] // shards_of).reshape((-1,) + (1,) * (len(dims) - axis_at - 1))

    factor_of = one(*cuts[0])
    for cut in cuts[1:]:
        factor_of = factor_of * one(*cut)
    return factor_of


def normal_values(key, extent, spread, reach, cuts=(), kind=jnp.bfloat16):
    entries = jax.random.normal(key, extent, jnp.float32) * spread
    if len(cuts) > 0:
        entries = shard_levels(key, extent, cuts, -0.22, 0.18) * entries
    return jnp.clip(entries, min=-reach, max=reach).astype(kind)


def setup_inputs(seed: int = 0) -> dict:
    streams_of = jax.random.split(jax.random.key(seed), 4)
    return {
        "fields": normal_values(streams_of[0], (COLS, FIELDS * LEV), 1.0, 6.0, ((0, 32),), jnp.float32),
        "file_offset": draw_file_offset(jax.random.fold_in(streams_of[3], 71), 0),
        "level_remap": normal_values(streams_of[2], (FIELDS, LEV, LEV), LEV ** -0.5, 0.75, (), jnp.float32),
    }


def reference(fields, file_offset, level_remap):
    columns = fields.shape[0]
    shaped = fields.reshape(columns, FIELDS, LEV)
    mixed = jnp.einsum("cfl,flm->cfm", shaped, level_remap, precision=lax.Precision.HIGHEST)
    remapped = mixed.reshape(columns, FIELDS * LEV)
    positions = file_offset.reshape(columns).astype(jnp.int32)
    history = jnp.zeros_like(remapped).at[positions].set(remapped)
    return history
```

```python
import functools

import jax
import jax.numpy as jnp
from jax import lax
from jax.experimental import pallas as pl
from jax.experimental.pallas import tpu as pltpu
from jax.sharding import PartitionSpec as P

SPREAD = 8
MOST = 192
NEAR = SPREAD + MOST
NEAR_ROWS = -(-NEAR // 128)
LIMIT = 24 * 1024 * 1024
I32 = jnp.int32
F32 = jnp.float32
BF16 = jnp.bfloat16


def whole_part(value, divisor):
    return ((value.astype(F32) + 0.5) * (1.0 / divisor)).astype(I32)


def view_row(row):
    return ((row >> 3) << 4) + (row & 7)


def route_kernel(n_io, n_comp, off_ref, src_ref, near_ref, far_ref):
    rows = off_ref.shape[0]
    columns = rows * 128
    far = far_ref.shape[0]
    kinds = 4 + far
    my_group = lax.axis_index("io")
    my_task = lax.axis_index("comp")
    offset = off_ref[...]
    owner = whole_part(offset, columns)
    place = offset - owner * columns
    group = whole_part(owner, n_comp)
    task = owner - group * n_comp
    step_c = task - my_task
    step_c = jnp.where(step_c < 0, step_c + n_comp, step_c)
    step_g = group - my_group
    step_g = jnp.where(step_g < 0, step_g + n_io, step_g)
    kind_c = jnp.where(step_c == 1, 0, jnp.where(step_c == n_comp - 1, 1, step_c + 2))
    kind_g = jnp.where(
        step_g == 1, 2, jnp.where(step_g == n_io - 1, 3, step_g + (2 + n_comp - 3))
    )
    stays = (step_c == 0) & (step_g == 0)
    kind = jnp.where(stays, -1, jnp.where(step_g == 0, kind_c, kind_g))

    masks = [(kind == k).astype(F32) for k in range(kinds)]
    stacked = jnp.concatenate(masks, axis=0).astype(BF16)
    r2 = lax.broadcasted_iota(I32, (128, 256), 0)
    c2 = lax.broadcasted_iota(I32, (128, 256), 1)
    tri = ((c2 >= 128) | (r2 < c2)).astype(F32).astype(BF16)
    both = jnp.dot(stacked, tri, preferred_element_type=F32)
    totals = jnp.concatenate(
        [both[k * rows : (k + 1) * rows, 128:] for k in range(kinds)], axis=1
    ).astype(BF16)
    lr = lax.broadcasted_iota(I32, (rows, rows), 0)
    lc = lax.broadcasted_iota(I32, (rows, rows), 1)
    lower = (lr > lc).astype(F32).astype(BF16)
    before = jnp.dot(lower, totals, preferred_element_type=F32)
    rank = jnp.zeros((rows, 128), F32)
    for k in range(kinds):
        rank += masks[k] * (
            both[k * rows : (k + 1) * rows, :128] + before[:, k * 128 : (k + 1) * 128]
        )
    rank = rank.astype(I32)

    base = jnp.where(kind < 4, rows + NEAR_ROWS * kind, rows + (NEAR_ROWS - 1) * 4 + kind)
    high = jnp.where(stays, place >> 7, base + (rank >> 7))
    low = jnp.where(stays, place & 127, rank & 127)
    place_high = (place >> 7).astype(F32) + 1.0
    place_low = (place & 127).astype(F32)

    total = src_ref.shape[0]
    hi_iota = lax.broadcasted_iota(I32, (total, 128), 0)
    lane_iota = lax.broadcasted_iota(I32, (total, 128), 1).astype(F32)
    lo_iota = lax.broadcasted_iota(I32, (128, 128), 0)
    acc = jnp.zeros((4 * total, 128), F32)
    for r in range(rows):
        hit = (hi_iota == high[r : r + 1, :]).astype(F32)
        left = jnp.concatenate(
            [
                hit * float(r),
                hit * lane_iota,
                hit * place_high[r : r + 1, :],
                hit * place_low[r : r + 1, :],
            ],
            axis=0,
        ).astype(BF16)
        right = (lo_iota == low[r : r + 1, :]).astype(F32).astype(BF16)
        acc += lax.dot_general(
            left, right, (((1,), (1,)), ((), ())), preferred_element_type=F32
        )
    found = acc.astype(I32)
    src_ref[...] = view_row(found[:total] * 128 + found[total : 2 * total])
    p_high = found[2 * total : 3 * total]
    target = (p_high - 1) * 128 + found[3 * total :]
    target = jnp.where(p_high > 0, view_row(target), 2 * columns)
    for k in range(4):
        near_ref[k] = target[rows + NEAR_ROWS * k : rows + NEAR_ROWS * (k + 1)]
    for j in range(far):
        at = rows + NEAR_ROWS * 4 + j
        far_ref[j] = target[at : at + 1]


def partners(n_io, n_comp):
    near = [("comp", 1), ("comp", n_comp - 1), ("io", 1), ("io", n_io - 1)]
    far = [("comp", d) for d in range(2, n_comp - 1)] + [("io", d) for d in range(2, n_io - 1)]
    return near, far


def mix(rows, weights):
    m = rows.shape[0] // 16
    parts = rows.reshape(m, 2, 8, 128)
    outs = []
    for h in range(2):
        x = parts[:, h].reshape(8 * m, 128)
        head = x.astype(BF16)
        tail = (x - head.astype(F32)).astype(BF16)
        y = jnp.dot(
            jnp.concatenate([head, tail], axis=1), weights[h], preferred_element_type=F32
        )
        outs.append((y[:, :128] + y[:, 128:]).reshape(m, 1, 8, 128))
    return jnp.concatenate(outs, axis=1).reshape(16 * m, 128)


def exchange_kernel(
    n_io,
    n_comp,
    src_ref,
    near_ref,
    far_ref,
    fields_ref,
    map_ref,
    block_ref,
    got_ref,
    near_out,
    far_out,
    send,
    recv,
    near_in,
    far_in,
    wide,
    row_send,
    row_recv,
    pos_send,
    pos_recv,
):
    view = fields_ref.shape[0]
    columns = view // 2
    near, far = partners(n_io, n_comp)
    sizes = {"io": n_io, "comp": n_comp}
    where = {"io": lax.axis_index("io"), "comp": lax.axis_index("comp")}

    def device(axis, step):
        return {axis: lax.rem(where[axis] + step, sizes[axis])}

    everyone = near + far
    barrier = pltpu.get_barrier_semaphore()
    for axis, step in everyone:
        pl.semaphore_signal(
            barrier, inc=1, device_id=device(axis, step), device_id_type=pl.DeviceIdType.MESH
        )

    def fetch(count, source, target, target_ref):
        def body(i, carry):
            got = [
                fields_ref[pl.ds(src_ref[source + i * 8 + s], 2, stride=8), :] for s in range(8)
            ]
            for s in range(8):
                target_ref[pl.ds(target + i * 16 + s, 2, stride=8), :] = got[s]
            return carry

        lax.fori_loop(0, count // 8, body, 0)

    copies = []

    def ship(source, target, sem_at, axis, step, sends, recvs):
        copy = pltpu.make_async_remote_copy(
            src_ref=source,
            dst_ref=target,
            send_sem=sends.at[sem_at],
            recv_sem=recvs.at[sem_at],
            device_id=device(axis, step),
            device_id_type=pl.DeviceIdType.MESH,
        )
        copy.start()
        copies.append(copy)

    for k in range(4):
        fetch(NEAR, columns + k * NEAR_ROWS * 128, k * 2 * NEAR, send)
        if k == 0:
            pl.semaphore_wait(barrier, len(everyone))
        axis, step = near[k]
        part = pl.ds(k * 2 * NEAR, 2 * NEAR)
        ship(send.at[part], recv.at[part], k, axis, step, row_send, row_recv)
    for j, (axis, step) in enumerate(far):
        start = 8 * NEAR + 16 * j
        fetch(8, columns + (4 * NEAR_ROWS + j) * 128, start, send)
        part = pl.ds(start, 16)
        ship(send.at[part], recv.at[part], 4 + j, axis, step, row_send, row_recv)
    for k, (axis, step) in enumerate(near):
        ship(near_ref.at[k], near_in.at[k], k, axis, step, pos_send, pos_recv)
    for j, (axis, step) in enumerate(far):
        ship(far_ref.at[j], far_in.at[j], 4 + j, axis, step, pos_send, pos_recv)

    weights = []
    for h in range(2):
        wide[...] = jnp.zeros((128, 128), F32)
        wide[:64, :64] = map_ref[2 * h]
        wide[64:, 64:] = map_ref[2 * h + 1]
        full = wide[...]
        head = full.astype(BF16)
        tail = (full - head.astype(F32)).astype(BF16)
        line = jnp.concatenate([head, tail], axis=1)
        weights.append(jnp.concatenate([line, line], axis=0))

    fetch(columns, 0, 0, block_ref)
    chunk = 512

    def mix_block(i, carry):
        at = pl.ds(i * chunk, chunk)
        block_ref[at, :] = mix(block_ref[at, :], weights)
        return carry

    lax.fori_loop(0, view // chunk, mix_block, 0)

    for copy in copies:
        copy.wait()
    for k in range(4):
        part = slice(k * 2 * NEAR, (k + 1) * 2 * NEAR)
        got_ref[part, :] = mix(recv[part, :], weights)
    part = slice(8 * NEAR, send.shape[0])
    got_ref[part, :] = mix(recv[part, :], weights)
    near_out[...] = near_in[...]
    far_out[...] = far_in[...]


def place_kernel(near_ref, far_ref, block_in, got_ref, block_ref, out_ref, sem):
    def put(count, source, index_ref, index):
        def body(i, carry):
            rows = [got_ref[pl.ds(source + i * 16 + s, 2, stride=8), :] for s in range(8)]
            for s in range(8):
                block_ref[pl.ds(index_ref[index + i * 8 + s], 2, stride=8), :] = rows[s]
            return carry

        lax.fori_loop(0, count // 8, body, 0)

    for k in range(4):
        put(NEAR, k * 2 * NEAR, near_ref, k * NEAR_ROWS * 128)
    for j in range(far_ref.shape[0] // 128):
        put(8, 8 * NEAR + 16 * j, far_ref, j * 128)
    copy = pltpu.make_async_copy(block_ref.at[pl.ds(0, out_ref.shape[0])], out_ref, sem)
    copy.start()
    copy.wait()


def per_device(fields, file_offset, level_remap):
    columns, width = fields.shape
    n_io = lax.axis_size("io")
    n_comp = lax.axis_size("comp")
    near, far = partners(n_io, n_comp)
    count = len(far)
    rows = file_offset.shape[0]
    total = -(-(rows + 4 * NEAR_ROWS + count) // 8) * 8
    vmem = pl.BlockSpec(memory_space=pltpu.VMEM)
    smem = pl.BlockSpec(memory_space=pltpu.SMEM)
    hbm = pl.BlockSpec(memory_space=pl.ANY)

    src, near_pos, far_pos = pl.pallas_call(
        functools.partial(route_kernel, n_io, n_comp),
        out_shape=(
            jax.ShapeDtypeStruct((total, 128), I32),
            jax.ShapeDtypeStruct((4, NEAR_ROWS, 128), I32),
            jax.ShapeDtypeStruct((count, 1, 128), I32),
        ),
        in_specs=[vmem],
        out_specs=(vmem,) * 3,
        compiler_params=pltpu.CompilerParams(vmem_limit_bytes=LIMIT),
        name="route",
    )(file_offset)

    view = fields.reshape(columns // 8, 8, 2, 128).transpose(0, 2, 1, 3).reshape(2 * columns, 128)
    slots = 4 * NEAR + 8 * count
    kinds = 4 + count
    block, got, near_got, far_got = pl.pallas_call(
        functools.partial(exchange_kernel, n_io, n_comp),
        out_shape=(
            pltpu.VMEM((2 * columns + 16, 128), F32),
            jax.ShapeDtypeStruct((2 * slots, 128), F32),
            jax.ShapeDtypeStruct((4, NEAR_ROWS, 128), I32),
            jax.ShapeDtypeStruct((count, 1, 128), I32),
        ),
        in_specs=[smem, vmem, vmem, vmem, vmem],
        out_specs=(vmem,) * 4,
        scratch_shapes=[
            pltpu.VMEM((2 * slots, 128), F32),
            pltpu.VMEM((2 * slots, 128), F32),
            pltpu.VMEM((4, NEAR_ROWS, 128), I32),
            pltpu.VMEM((count, 1, 128), I32),
            pltpu.VMEM((128, 128), F32),
            pltpu.SemaphoreType.DMA((kinds,)),
            pltpu.SemaphoreType.DMA((kinds,)),
            pltpu.SemaphoreType.DMA((kinds,)),
            pltpu.SemaphoreType.DMA((kinds,)),
        ],
        compiler_params=pltpu.CompilerParams(
            collective_id=0, has_side_effects=True, vmem_limit_bytes=LIMIT
        ),
        name="exchange",
    )(src.reshape(-1), near_pos, far_pos, view, level_remap)

    _, out = pl.pallas_call(
        place_kernel,
        out_shape=(
            pltpu.VMEM(block.shape, F32),
            jax.ShapeDtypeStruct((2 * columns, 128), F32),
        ),
        in_specs=[smem, smem, vmem, vmem],
        out_specs=(vmem, hbm),
        scratch_shapes=[pltpu.SemaphoreType.DMA],
        input_output_aliases={2: 0},
        compiler_params=pltpu.CompilerParams(vmem_limit_bytes=LIMIT),
        name="place",
    )(near_got.reshape(-1), far_got.reshape(-1), block, got)
    return out.reshape(columns // 8, 2, 8, 128).transpose(0, 2, 1, 3).reshape(columns, width)


def solution(mesh):
    placed = (P(("io", "comp"), None), P(("io", "comp"), None), P())
    return jax.shard_map(
        per_device, mesh=mesh, in_specs=placed, out_specs=P(("io", "comp"), None), check_vma=False
    )
```

```python
import functools

import jax
import jax.numpy as jnp
from jax import lax
from jax.experimental import pallas as pl
from jax.experimental.pallas import tpu as pltpu
from jax.sharding import PartitionSpec as P

SPREAD = 8
MOST = 192
NEAR = SPREAD + MOST
NEAR_ROWS = -(-NEAR // 128)
PIECES = 4
LIMIT = 24 * 1024 * 1024
I32 = jnp.int32
F32 = jnp.float32
BF16 = jnp.bfloat16


def whole_part(value, divisor):
    return ((value.astype(F32) + 0.5) * (1.0 / divisor)).astype(I32)


def view_row(row):
    return ((row >> 3) << 4) + (row & 7)


def route_kernel(
    n_io,
    n_comp,
    off_hbm,
    fields_hbm,
    map_hbm,
    src_ref,
    near_ref,
    far_ref,
    fields_ref,
    weight_ref,
    off_ref,
    map_ref,
    wide,
    sems,
):
    rows = off_ref.shape[0]
    off_copy = pltpu.make_async_copy(off_hbm, off_ref, sems.at[PIECES])
    off_copy.start()
    piece = fields_ref.shape[0] // PIECES
    loads = [
        pltpu.make_async_copy(
            fields_hbm.at[pl.ds(i * piece, piece)],
            fields_ref.at[pl.ds(i * piece, piece)],
            sems.at[i],
        )
        for i in range(PIECES)
    ]
    for load in loads:
        load.start()
    map_copy = pltpu.make_async_copy(map_hbm, map_ref, sems.at[PIECES + 1])
    map_copy.start()
    off_copy.wait()
    columns = rows * 128
    far = far_ref.shape[0]
    kinds = 4 + far
    my_group = lax.axis_index("io")
    my_task = lax.axis_index("comp")
    offset = off_ref[...]
    owner = whole_part(offset, columns)
    place = offset - owner * columns
    group = whole_part(owner, n_comp)
    task = owner - group * n_comp
    step_c = task - my_task
    step_c = jnp.where(step_c < 0, step_c + n_comp, step_c)
    step_g = group - my_group
    step_g = jnp.where(step_g < 0, step_g + n_io, step_g)
    kind_c = jnp.where(step_c == 1, 0, jnp.where(step_c == n_comp - 1, 1, step_c + 2))
    kind_g = jnp.where(
        step_g == 1, 2, jnp.where(step_g == n_io - 1, 3, step_g + (2 + n_comp - 3))
    )
    stays = (step_c == 0) & (step_g == 0)
    kind = jnp.where(stays, -1, jnp.where(step_g == 0, kind_c, kind_g))

    masks = [(kind == k).astype(F32) for k in range(kinds)]
    stacked = jnp.concatenate(masks, axis=0).astype(BF16)
    r2 = lax.broadcasted_iota(I32, (128, 256), 0)
    c2 = lax.broadcasted_iota(I32, (128, 256), 1)
    tri = ((c2 >= 128) | (r2 < c2)).astype(F32).astype(BF16)
    both = jnp.dot(stacked, tri, preferred_element_type=F32)
    totals = jnp.concatenate(
        [both[k * rows : (k + 1) * rows, 128:] for k in range(kinds)], axis=1
    ).astype(BF16)
    lr = lax.broadcasted_iota(I32, (rows, rows), 0)
    lc = lax.broadcasted_iota(I32, (rows, rows), 1)
    lower = (lr > lc).astype(F32).astype(BF16)
    before = jnp.dot(lower, totals, preferred_element_type=F32)
    rank = jnp.zeros((rows, 128), F32)
    for k in range(kinds):
        rank += masks[k] * (
            both[k * rows : (k + 1) * rows, :128] + before[:, k * 128 : (k + 1) * 128]
        )
    rank = rank.astype(I32)

    base = jnp.where(kind < 4, rows + NEAR_ROWS * kind, rows + (NEAR_ROWS - 1) * 4 + kind)
    high = jnp.where(stays, place >> 7, base + (rank >> 7))
    low = jnp.where(stays, place & 127, rank & 127)
    place_high = (place >> 7).astype(F32) + 1.0
    place_low = (place & 127).astype(F32)

    total = src_ref.shape[0]
    hi_iota = lax.broadcasted_iota(I32, (total, 128), 0)
    lane_iota = lax.broadcasted_iota(I32, (total, 128), 1).astype(F32)
    lo_iota = lax.broadcasted_iota(I32, (128, 128), 0)
    acc = jnp.zeros((4 * total, 128), F32)
    for r in range(rows):
        hit = (hi_iota == high[r : r + 1, :]).astype(F32)
        left = jnp.concatenate(
            [
                hit * float(r),
                hit * lane_iota,
                hit * place_high[r : r + 1, :],
                hit * place_low[r : r + 1, :],
            ],
            axis=0,
        ).astype(BF16)
        right = (lo_iota == low[r : r + 1, :]).astype(F32).astype(BF16)
        acc += lax.dot_general(
            left, right, (((1,), (1,)), ((), ())), preferred_element_type=F32
        )
    found = acc.astype(I32)
    src_ref[...] = view_row(found[:total] * 128 + found[total : 2 * total])
    p_high = found[2 * total : 3 * total]
    target = (p_high - 1) * 128 + found[3 * total :]
    target = jnp.where(p_high > 0, view_row(target), 2 * columns)
    for k in range(4):
        near_ref[k] = target[rows + NEAR_ROWS * k : rows + NEAR_ROWS * (k + 1)]
    for j in range(far):
        at = rows + NEAR_ROWS * 4 + j
        far_ref[j] = target[at : at + 1]

    map_copy.wait()
    for h in range(2):
        wide[...] = jnp.zeros((128, 128), F32)
        wide[:64, :64] = map_ref[2 * h]
        wide[64:, 64:] = map_ref[2 * h + 1]
        full = wide[...]
        head = full.astype(BF16)
        tail = (full - head.astype(F32)).astype(BF16)
        line = jnp.concatenate([head, tail], axis=1)
        weight_ref[h] = jnp.concatenate([line, line], axis=0)
    for load in loads:
        load.wait()


def partners(n_io, n_comp):
    near = [("comp", 1), ("comp", n_comp - 1), ("io", 1), ("io", n_io - 1)]
    far = [("comp", d) for d in range(2, n_comp - 1)] + [("io", d) for d in range(2, n_io - 1)]
    return near, far


def mix(rows, weights):
    m = rows.shape[0] // 16
    parts = rows.reshape(m, 2, 8, 128)
    outs = []
    for h in range(2):
        x = parts[:, h].reshape(8 * m, 128)
        head = x.astype(BF16)
        tail = (x - head.astype(F32)).astype(BF16)
        y = jnp.dot(
            jnp.concatenate([head, tail], axis=1), weights[h], preferred_element_type=F32
        )
        outs.append((y[:, :128] + y[:, 128:]).reshape(m, 1, 8, 128))
    return jnp.concatenate(outs, axis=1).reshape(16 * m, 128)


def exchange_kernel(
    n_io,
    n_comp,
    src_ref,
    near_ref,
    far_ref,
    fields_ref,
    weight_ref,
    block_ref,
    near_out,
    far_out,
    send,
    recv,
    near_in,
    far_in,
    row_send,
    row_recv,
    pos_send,
    pos_recv,
):
    view = fields_ref.shape[0]
    columns = view // 2
    near, far = partners(n_io, n_comp)
    sizes = {"io": n_io, "comp": n_comp}
    where = {"io": lax.axis_index("io"), "comp": lax.axis_index("comp")}

    def device(axis, step):
        return {axis: lax.rem(where[axis] + step, sizes[axis])}

    everyone = near + far
    barrier = pltpu.get_barrier_semaphore()
    for axis, step in everyone:
        pl.semaphore_signal(
            barrier, inc=1, device_id=device(axis, step), device_id_type=pl.DeviceIdType.MESH
        )

    def fetch(count, source, target, target_ref):
        def body(i, carry):
            got = [
                fields_ref[pl.ds(src_ref[source + i * 8 + s], 2, stride=8), :] for s in range(8)
            ]
            for s in range(8):
                target_ref[pl.ds(target + i * 16 + s, 2, stride=8), :] = got[s]
            return carry

        lax.fori_loop(0, count // 8, body, 0)

    copies = []

    def ship(source, target, sem_at, axis, step, sends, recvs):
        copy = pltpu.make_async_remote_copy(
            src_ref=source,
            dst_ref=target,
            send_sem=sends.at[sem_at],
            recv_sem=recvs.at[sem_at],
            device_id=device(axis, step),
            device_id_type=pl.DeviceIdType.MESH,
        )
        copy.start()
        copies.append(copy)

    for k in range(4):
        fetch(NEAR, columns + k * NEAR_ROWS * 128, k * 2 * NEAR, send)
        if k == 0:
            pl.semaphore_wait(barrier, len(everyone))
        axis, step = near[k]
        part = pl.ds(k * 2 * NEAR, 2 * NEAR)
        ship(send.at[part], recv.at[part], k, axis, step, row_send, row_recv)
    for j, (axis, step) in enumerate(far):
        start = 8 * NEAR + 16 * j
        fetch(8, columns + (4 * NEAR_ROWS + j) * 128, start, send)
        part = pl.ds(start, 16)
        ship(send.at[part], recv.at[part], 4 + j, axis, step, row_send, row_recv)
    for k, (axis, step) in enumerate(near):
        ship(near_ref.at[k], near_in.at[k], k, axis, step, pos_send, pos_recv)
    for j, (axis, step) in enumerate(far):
        ship(far_ref.at[j], far_in.at[j], 4 + j, axis, step, pos_send, pos_recv)

    weights = [weight_ref[0], weight_ref[1]]
    fetch(columns, 0, 0, block_ref)
    chunk = 512

    def mix_block(i, carry):
        at = pl.ds(i * chunk, chunk)
        block_ref[at, :] = mix(block_ref[at, :], weights)
        return carry

    lax.fori_loop(0, view // chunk, mix_block, 0)

    got = view + 16

    def mix_got(first, last):
        block_ref[got + first : got + last, :] = mix(recv[first:last, :], weights)

    for copy in copies[4:]:
        copy.wait()
    mix_got(8 * NEAR, send.shape[0])
    for k in (2, 3, 0, 1):
        copies[k].wait()
        mix_got(k * 2 * NEAR, (k + 1) * 2 * NEAR)
    near_out[...] = near_in[...]
    far_out[...] = far_in[...]


def place_kernel(near_ref, far_ref, block_in, block_ref, out_ref, sems):
    view = out_ref.shape[0]
    got = view + 16

    def put(count, source, index_at):
        def body(i, carry):
            rows = [block_ref[pl.ds(got + source + i * 16 + s, 2, stride=8), :] for s in range(8)]
            for s in range(8):
                block_ref[pl.ds(index_at(i * 8 + s), 2, stride=8), :] = rows[s]
            return carry

        lax.fori_loop(0, count // 8, body, 0)

    for k in range(4):
        put(NEAR, k * 2 * NEAR, lambda i: near_ref[k * NEAR_ROWS * 128 + i])
    for j in range(far_ref.shape[0]):
        put(SPREAD, 8 * NEAR + 16 * j, lambda i: far_ref[j, 0, i])
    piece = view // PIECES
    stores = [
        pltpu.make_async_copy(
            block_ref.at[pl.ds(i * piece, piece)], out_ref.at[pl.ds(i * piece, piece)], sems.at[i]
        )
        for i in range(PIECES)
    ]
    for store in stores:
        store.start()
    for store in stores:
        store.wait()


def per_device(fields, file_offset, level_remap):
    columns, width = fields.shape
    n_io = lax.axis_size("io")
    n_comp = lax.axis_size("comp")
    near, far = partners(n_io, n_comp)
    count = len(far)
    rows = file_offset.shape[0]
    total = -(-(rows + 4 * NEAR_ROWS + count) // 8) * 8
    vmem = pl.BlockSpec(memory_space=pltpu.VMEM)
    smem = pl.BlockSpec(memory_space=pltpu.SMEM)
    hbm = pl.BlockSpec(memory_space=pltpu.HBM)

    view = fields.reshape(columns // 8, 8, 2, 128).transpose(0, 2, 1, 3).reshape(2 * columns, 128)
    src, near_pos, far_pos, held, weights = pl.pallas_call(
        functools.partial(route_kernel, n_io, n_comp),
        out_shape=(
            jax.ShapeDtypeStruct((total, 128), I32),
            jax.ShapeDtypeStruct((4, NEAR_ROWS, 128), I32),
            jax.ShapeDtypeStruct((count, 1, 128), I32),
            pltpu.VMEM((2 * columns, 128), F32),
            pltpu.VMEM((2, 256, 256), BF16),
        ),
        in_specs=[hbm, hbm, hbm],
        out_specs=(vmem,) * 5,
        scratch_shapes=[
            pltpu.VMEM(file_offset.shape, I32),
            pltpu.VMEM(level_remap.shape, F32),
            pltpu.VMEM((128, 128), F32),
            pltpu.SemaphoreType.DMA((PIECES + 2,)),
        ],
        compiler_params=pltpu.CompilerParams(vmem_limit_bytes=LIMIT),
        name="route",
    )(*[pltpu.with_memory_space_constraint(x, pltpu.HBM) for x in (file_offset, view, level_remap)])

    slots = 4 * NEAR + 8 * count
    kinds = 4 + count
    block, near_got, far_got = pl.pallas_call(
        functools.partial(exchange_kernel, n_io, n_comp),
        out_shape=(
            pltpu.VMEM((2 * columns + 16 + 2 * slots, 128), F32),
            jax.ShapeDtypeStruct((4, NEAR_ROWS, 128), I32),
            jax.ShapeDtypeStruct((count, 1, 128), I32),
        ),
        in_specs=[smem, vmem, vmem, vmem, vmem],
        out_specs=(vmem,) * 3,
        scratch_shapes=[
            pltpu.VMEM((2 * slots, 128), F32),
            pltpu.VMEM((2 * slots, 128), F32),
            pltpu.VMEM((4, NEAR_ROWS, 128), I32),
            pltpu.VMEM((count, 1, 128), I32),
            pltpu.SemaphoreType.DMA((kinds,)),
            pltpu.SemaphoreType.DMA((kinds,)),
            pltpu.SemaphoreType.DMA((kinds,)),
            pltpu.SemaphoreType.DMA((kinds,)),
        ],
        compiler_params=pltpu.CompilerParams(
            collective_id=0, has_side_effects=True, vmem_limit_bytes=LIMIT
        ),
        name="exchange",
    )(src.reshape(-1), near_pos, far_pos, held, weights)

    _, out = pl.pallas_call(
        place_kernel,
        out_shape=(
            pltpu.VMEM(block.shape, F32),
            jax.ShapeDtypeStruct((2 * columns, 128), F32),
        ),
        in_specs=[smem, smem, vmem],
        out_specs=(vmem, hbm),
        scratch_shapes=[pltpu.SemaphoreType.DMA((PIECES,))],
        input_output_aliases={2: 0},
        compiler_params=pltpu.CompilerParams(vmem_limit_bytes=LIMIT),
        name="place",
    )(near_got.reshape(-1), far_got, block)
    return out.reshape(columns // 8, 2, 8, 128).transpose(0, 2, 1, 3).reshape(columns, width)


def solution(mesh):
    placed = (P(("io", "comp"), None), P(("io", "comp"), None), P())
    return jax.shard_map(
        per_device, mesh=mesh, in_specs=placed, out_specs=P(("io", "comp"), None), check_vma=False
    )
```

```python
import functools

import jax
import jax.numpy as jnp
from jax import lax
from jax.experimental import pallas as pl
from jax.experimental.pallas import tpu as pltpu
from jax.sharding import PartitionSpec as P

SPREAD = 8
MOST = 192
NEAR = SPREAD + MOST
NEAR_ROWS = -(-NEAR // 128)
PIECES = 4
LIMIT = 24 * 1024 * 1024
I32 = jnp.int32
F32 = jnp.float32
BF16 = jnp.bfloat16


def whole_part(value, divisor):
    return ((value.astype(F32) + 0.5) * (1.0 / divisor)).astype(I32)


def view_row(row):
    return ((row >> 3) << 4) + (row & 7)


def route_kernel(
    n_io,
    n_comp,
    off_hbm,
    fields_hbm,
    map_hbm,
    src_ref,
    near_ref,
    far_ref,
    fields_ref,
    weight_ref,
    off_ref,
    map_ref,
    wide,
    sems,
):
    rows = off_ref.shape[0]
    off_copy = pltpu.make_async_copy(off_hbm, off_ref, sems.at[PIECES])
    off_copy.start()
    piece = fields_ref.shape[0] // PIECES
    loads = [
        pltpu.make_async_copy(
            fields_hbm.at[pl.ds(i * piece, piece)],
            fields_ref.at[pl.ds(i * piece, piece)],
            sems.at[i],
        )
        for i in range(PIECES)
    ]
    for load in loads:
        load.start()
    map_copy = pltpu.make_async_copy(map_hbm, map_ref, sems.at[PIECES + 1])
    map_copy.start()
    off_copy.wait()
    columns = rows * 128
    far = far_ref.shape[0]
    kinds = 4 + far
    my_group = lax.axis_index("io")
    my_task = lax.axis_index("comp")
    offset = off_ref[...]
    owner = whole_part(offset, columns)
    place = offset - owner * columns
    group = whole_part(owner, n_comp)
    task = owner - group * n_comp
    step_c = task - my_task
    step_c = jnp.where(step_c < 0, step_c + n_comp, step_c)
    step_g = group - my_group
    step_g = jnp.where(step_g < 0, step_g + n_io, step_g)
    kind_c = jnp.where(step_c == 1, 0, jnp.where(step_c == n_comp - 1, 1, step_c + 2))
    kind_g = jnp.where(
        step_g == 1, 2, jnp.where(step_g == n_io - 1, 3, step_g + (2 + n_comp - 3))
    )
    stays = (step_c == 0) & (step_g == 0)
    kind = jnp.where(stays, -1, jnp.where(step_g == 0, kind_c, kind_g))

    masks = [(kind == k).astype(F32) for k in range(kinds)]
    stacked = jnp.concatenate(masks, axis=0).astype(BF16)
    r2 = lax.broadcasted_iota(I32, (128, 256), 0)
    c2 = lax.broadcasted_iota(I32, (128, 256), 1)
    tri = ((c2 >= 128) | (r2 < c2)).astype(F32).astype(BF16)
    both = jnp.dot(stacked, tri, preferred_element_type=F32)
    totals = jnp.concatenate(
        [both[k * rows : (k + 1) * rows, 128:] for k in range(kinds)], axis=1
    ).astype(BF16)
    lr = lax.broadcasted_iota(I32, (rows, rows), 0)
    lc = lax.broadcasted_iota(I32, (rows, rows), 1)
    lower = (lr > lc).astype(F32).astype(BF16)
    before = jnp.dot(lower, totals, preferred_element_type=F32)
    rank = jnp.zeros((rows, 128), F32)
    for k in range(kinds):
        rank += masks[k] * (
            both[k * rows : (k + 1) * rows, :128] + before[:, k * 128 : (k + 1) * 128]
        )
    rank = rank.astype(I32)

    base = jnp.where(kind < 4, rows + NEAR_ROWS * kind, rows + (NEAR_ROWS - 1) * 4 + kind)
    high = jnp.where(stays, place >> 7, base + (rank >> 7))
    low = jnp.where(stays, place & 127, rank & 127)
    place_high = (place >> 7).astype(F32) + 1.0
    place_low = (place & 127).astype(F32)

    total = src_ref.shape[0]
    hi_iota = lax.broadcasted_iota(I32, (total, 128), 0)
    lane_iota = lax.broadcasted_iota(I32, (total, 128), 1).astype(F32)
    lo_iota = lax.broadcasted_iota(I32, (128, 128), 0)
    acc = jnp.zeros((4 * total, 128), F32)
    for r in range(rows):
        hit = (hi_iota == high[r : r + 1, :]).astype(F32)
        left = jnp.concatenate(
            [
                hit * float(r),
                hit * lane_iota,
                hit * place_high[r : r + 1, :],
                hit * place_low[r : r + 1, :],
            ],
            axis=0,
        ).astype(BF16)
        right = (lo_iota == low[r : r + 1, :]).astype(F32).astype(BF16)
        acc += lax.dot_general(
            left, right, (((1,), (1,)), ((), ())), preferred_element_type=F32
        )
    found = acc.astype(I32)
    src_ref[...] = view_row(found[:total] * 128 + found[total : 2 * total])
    p_high = found[2 * total : 3 * total]
    target = (p_high - 1) * 128 + found[3 * total :]
    target = jnp.where(p_high > 0, view_row(target), 2 * columns)
    for k in range(4):
        near_ref[k] = target[rows + NEAR_ROWS * k : rows + NEAR_ROWS * (k + 1)]
    for j in range(far):
        at = rows + NEAR_ROWS * 4 + j
        far_ref[j] = target[at : at + 1]

    map_copy.wait()
    for h in range(2):
        wide[...] = jnp.zeros((128, 128), F32)
        wide[:64, :64] = map_ref[2 * h]
        wide[64:, 64:] = map_ref[2 * h + 1]
        full = wide[...]
        head = full.astype(BF16)
        tail = (full - head.astype(F32)).astype(BF16)
        line = jnp.concatenate([head, tail], axis=1)
        weight_ref[h] = jnp.concatenate([line, line], axis=0)
    for load in loads:
        load.wait()


def partners(n_io, n_comp):
    near = [("comp", 1), ("comp", n_comp - 1), ("io", 1), ("io", n_io - 1)]
    far = [("comp", d) for d in range(2, n_comp - 1)] + [("io", d) for d in range(2, n_io - 1)]
    return near, far


def mix(rows, weights):
    m = rows.shape[0] // 16
    parts = rows.reshape(m, 2, 8, 128)
    outs = []
    for h in range(2):
        x = parts[:, h].reshape(8 * m, 128)
        head = x.astype(BF16)
        tail = (x - head.astype(F32)).astype(BF16)
        y = jnp.dot(
            jnp.concatenate([head, tail], axis=1), weights[h], preferred_element_type=F32
        )
        outs.append((y[:, :128] + y[:, 128:]).reshape(m, 1, 8, 128))
    return jnp.concatenate(outs, axis=1).reshape(16 * m, 128)


def exchange_kernel(
    n_io,
    n_comp,
    src_ref,
    near_ref,
    far_ref,
    fields_ref,
    weight_ref,
    block_ref,
    near_out,
    far_out,
    send,
    recv,
    near_in,
    far_in,
    row_send,
    row_recv,
    pos_send,
    pos_recv,
):
    view = fields_ref.shape[0]
    columns = view // 2
    near, far = partners(n_io, n_comp)
    sizes = {"io": n_io, "comp": n_comp}
    where = {"io": lax.axis_index("io"), "comp": lax.axis_index("comp")}

    def device(axis, step):
        return {axis: lax.rem(where[axis] + step, sizes[axis])}

    everyone = near + far
    barrier = pltpu.get_barrier_semaphore()
    for axis, step in everyone:
        pl.semaphore_signal(
            barrier, inc=1, device_id=device(axis, step), device_id_type=pl.DeviceIdType.MESH
        )

    def fetch(count, source, target, target_ref):
        lines = 5 if count % 40 == 0 else 4 if count % 32 == 0 else 1

        def body(i, carry):
            got = []
            for s in range(8 * lines):
                at = source + i * 8 * lines + s
                got.append(fields_ref[pl.ds(src_ref[at], 2, stride=8), :])
            for s in range(8 * lines):
                to = target + i * 16 * lines + 16 * (s // 8) + s % 8
                target_ref[pl.ds(to, 2, stride=8), :] = got[s]
            return carry

        lax.fori_loop(0, count // (8 * lines), body, 0)

    def ship(source, target, sem_at, axis, step, sends, recvs):
        copy = pltpu.make_async_remote_copy(
            src_ref=source,
            dst_ref=target,
            send_sem=sends.at[sem_at],
            recv_sem=recvs.at[sem_at],
            device_id=device(axis, step),
            device_id_type=pl.DeviceIdType.MESH,
        )
        copy.start()
        return copy

    def ship_near(k):
        fetch(NEAR, columns + k * NEAR_ROWS * 128, k * 2 * NEAR, send)
        if k == 0:
            pl.semaphore_wait(barrier, len(everyone))
        axis, step = near[k]
        part = pl.ds(k * 2 * NEAR, 2 * NEAR)
        return ship(send.at[part], recv.at[part], k, axis, step, row_send, row_recv)

    near_copies = [ship_near(0), ship_near(1)]
    small = []
    for k, (axis, step) in enumerate(near):
        small.append(ship(near_ref.at[k], near_in.at[k], k, axis, step, pos_send, pos_recv))
    for j, (axis, step) in enumerate(far):
        small.append(ship(far_ref.at[j], far_in.at[j], 4 + j, axis, step, pos_send, pos_recv))
        start = 8 * NEAR + 16 * j
        fetch(8, columns + (4 * NEAR_ROWS + j) * 128, start, send)
        part = pl.ds(start, 16)
        small.append(ship(send.at[part], recv.at[part], 4 + j, axis, step, row_send, row_recv))
    near_copies += [ship_near(2), ship_near(3)]

    weights = [weight_ref[0], weight_ref[1]]
    fetch(columns, 0, 0, block_ref)
    chunk = 512

    def mix_block(i, carry):
        at = pl.ds(i * chunk, chunk)
        block_ref[at, :] = mix(block_ref[at, :], weights)
        return carry

    lax.fori_loop(0, view // chunk, mix_block, 0)

    got = view + 16

    def mix_got(first, last):
        block_ref[got + first : got + last, :] = mix(recv[first:last, :], weights)

    for copy in small:
        copy.wait()
    mix_got(8 * NEAR, send.shape[0])
    for k in (2, 3, 0, 1):
        near_copies[k].wait()
        mix_got(k * 2 * NEAR, (k + 1) * 2 * NEAR)
    near_out[...] = near_in[...]
    far_out[...] = far_in[...]


def place_kernel(near_ref, far_ref, block_in, block_ref, out_ref, sems):
    view = out_ref.shape[0]
    got = view + 16

    def put(count, source, index_at):
        lines = 5 if count % 40 == 0 else 1

        def body(i, carry):
            for t in range(lines):
                at = i * lines + t
                rows = [block_ref[pl.ds(got + source + at * 16 + s, 2, stride=8), :] for s in range(8)]
                for s in range(8):
                    block_ref[pl.ds(index_at(at * 8 + s), 2, stride=8), :] = rows[s]
            return carry

        lax.fori_loop(0, count // (8 * lines), body, 0)

    for k in range(4):
        put(NEAR, k * 2 * NEAR, lambda i: near_ref[k * NEAR_ROWS * 128 + i])
    for j in range(far_ref.shape[0]):
        put(SPREAD, 8 * NEAR + 16 * j, lambda i: far_ref[j, 0, i])
    piece = view // PIECES
    stores = [
        pltpu.make_async_copy(
            block_ref.at[pl.ds(i * piece, piece)], out_ref.at[pl.ds(i * piece, piece)], sems.at[i]
        )
        for i in range(PIECES)
    ]
    for store in stores:
        store.start()
    for store in stores:
        store.wait()


def per_device(fields, file_offset, level_remap):
    columns, width = fields.shape
    n_io = lax.axis_size("io")
    n_comp = lax.axis_size("comp")
    near, far = partners(n_io, n_comp)
    count = len(far)
    rows = file_offset.shape[0]
    total = -(-(rows + 4 * NEAR_ROWS + count) // 8) * 8
    vmem = pl.BlockSpec(memory_space=pltpu.VMEM)
    smem = pl.BlockSpec(memory_space=pltpu.SMEM)
    hbm = pl.BlockSpec(memory_space=pltpu.HBM)

    view = fields.reshape(columns // 8, 8, 2, 128).transpose(0, 2, 1, 3).reshape(2 * columns, 128)
    src, near_pos, far_pos, held, weights = pl.pallas_call(
        functools.partial(route_kernel, n_io, n_comp),
        out_shape=(
            jax.ShapeDtypeStruct((total, 128), I32),
            jax.ShapeDtypeStruct((4, NEAR_ROWS, 128), I32),
            jax.ShapeDtypeStruct((count, 1, 128), I32),
            pltpu.VMEM((2 * columns, 128), F32),
            pltpu.VMEM((2, 256, 256), BF16),
        ),
        in_specs=[hbm, hbm, hbm],
        out_specs=(vmem,) * 5,
        scratch_shapes=[
            pltpu.VMEM(file_offset.shape, I32),
            pltpu.VMEM(level_remap.shape, F32),
            pltpu.VMEM((128, 128), F32),
            pltpu.SemaphoreType.DMA((PIECES + 2,)),
        ],
        compiler_params=pltpu.CompilerParams(vmem_limit_bytes=LIMIT),
        name="route",
    )(*[pltpu.with_memory_space_constraint(x, pltpu.HBM) for x in (file_offset, view, level_remap)])

    slots = 4 * NEAR + 8 * count
    kinds = 4 + count
    block, near_got, far_got = pl.pallas_call(
        functools.partial(exchange_kernel, n_io, n_comp),
        out_shape=(
            pltpu.VMEM((2 * columns + 16 + 2 * slots, 128), F32),
            jax.ShapeDtypeStruct((4, NEAR_ROWS, 128), I32),
            jax.ShapeDtypeStruct((count, 1, 128), I32),
        ),
        in_specs=[smem, vmem, vmem, vmem, vmem],
        out_specs=(vmem,) * 3,
        scratch_shapes=[
            pltpu.VMEM((2 * slots, 128), F32),
            pltpu.VMEM((2 * slots, 128), F32),
            pltpu.VMEM((4, NEAR_ROWS, 128), I32),
            pltpu.VMEM((count, 1, 128), I32),
            pltpu.SemaphoreType.DMA((kinds,)),
            pltpu.SemaphoreType.DMA((kinds,)),
            pltpu.SemaphoreType.DMA((kinds,)),
            pltpu.SemaphoreType.DMA((kinds,)),
        ],
        compiler_params=pltpu.CompilerParams(
            collective_id=0, has_side_effects=True, vmem_limit_bytes=LIMIT
        ),
        name="exchange",
    )(src.reshape(-1), near_pos, far_pos, held, weights)

    _, out = pl.pallas_call(
        place_kernel,
        out_shape=(
            pltpu.VMEM(block.shape, F32),
            jax.ShapeDtypeStruct((2 * columns, 128), F32),
        ),
        in_specs=[smem, smem, vmem],
        out_specs=(vmem, hbm),
        scratch_shapes=[pltpu.SemaphoreType.DMA((PIECES,))],
        input_output_aliases={2: 0},
        compiler_params=pltpu.CompilerParams(vmem_limit_bytes=LIMIT),
        name="place",
    )(near_got.reshape(-1), far_got, block)
    return out.reshape(columns // 8, 2, 8, 128).transpose(0, 2, 1, 3).reshape(columns, width)


def solution(mesh):
    placed = (P(("io", "comp"), None), P(("io", "comp"), None), P())
    return jax.shard_map(
        per_device, mesh=mesh, in_specs=placed, out_specs=P(("io", "comp"), None), check_vma=False
    )
```
